512 devices in a mesh: layer: 4 (over x_hi, core), row: 8 (over y), col: 16 (over z, x_lo).
Axes of the slice: x: 4 (x_hi: 2, x_lo: 2; x = x_hi * 2 + x_lo), y: 8, z: 8, core: 2. Of those that a mesh axis runs over, the one named last changes fastest.
Arguments:
- front_pivot: bfloat16 [512, 256, 256], P(('layer', 'row', 'col')), may hold values from -8 to 40, as said below
- front_border: bfloat16 [512, 512, 256], P(('layer', 'row', 'col')), may hold values from -0.625 to 0.625
- pivot_live: int32 [512], P(('layer', 'row', 'col')), may hold values from 128 to 256
- rows_live: int32 [512, 4], P(('layer', 'row', 'col')), may hold values from 64 to 128
- border_block: int32 [512, 4], P(('layer', 'row', 'col')), may hold values from 0 to 63, as said below
- row_map: int32 [512, 4, 128], P(('layer', 'row', 'col')), may hold values from 0 to 127, each once within a row
- separator: float32 [8, 1024, 4, 2048], P(None, 'row', None, 'col'), may hold values from -16 to 32, as said below
Outputs:
- factored: float32 [8, 1024, 4, 2048], P('layer', 'row', None, 'col')
The draws below stay inside these ranges and needn't reach their ends.
Inputs may be any that keep to these rules, and one draw needn't show every extreme that they name: `front_pivot`: each leaf's pivot block is symmetric with a dominant diagonal. The separator's entries form a symmetric matrix that stays positive definite after the leaves' contributions are subtracted. `border_block`: the 4 blocks of one leaf are distinct. Among them no more than 1 leave the same remainder when divided by the number of grid rows, and no more than 1 the same remainder when divided by the number of grid columns; every leaf reaches both bounds. `row_map`: each group's entries are a permutation of 0 to 127. Pivot columns from pivot_live on are padding. Rows of a group from rows_live on are padding.
All inputs are finite; a program needn't handle non-finite values.
Results may differ from the reference program's by a relative error of at most 0.0003.
Values sent between devices are 32-bit elements; how exact they have to be, the bound alone decides.
A program may use at most 128 MiB of HBM per device.

```python
import jax
import jax.numpy as jnp
from jax import lax

NB = 128
P_SIZE = 256
GROUPS = 4
RL = 8
PANELS = 1
BORDER = 512
NBLK = 64
CL = 4
SEP = 8192
LEAVES = 512
N_ROW = 8
N_COL = 16
DEVICES = 512


def draw_front_pivot(key, part):
    noise_key, margin_key, across_key, downward_key = jax.random.split(jax.random.fold_in(key, 23), 4)
    grid_width = max(1, int(P_SIZE ** 0.5 + 0.5))
    noise_draw = jax.random.normal(noise_key, (LEAVES, P_SIZE, P_SIZE), jnp.float32)
    margin = jax.random.uniform(margin_key, (LEAVES, P_SIZE), jnp.float32, 1.5, 3.0)
    least_weight = 0.6931472
    most_weight = 1.7917595
    across = jnp.exp(jax.random.uniform(across_key, (LEAVES, P_SIZE), jnp.float32, least_weight, most_weight))
    downward = jnp.exp(jax.random.uniform(downward_key, (LEAVES, P_SIZE), jnp.float32, least_weight, most_weight))
    position = jnp.arange(P_SIZE)
    right_step = ((position[None, :] == position[:, None] + 1) & (position % grid_width < grid_width - 1)[:, None]).astype(jnp.float32)
    down_step = (position[None, :] == position[:, None] + grid_width).astype(jnp.float32)
    upper_part = across[:, :, None] * right_step[None, :, :] + downward[:, :, None] * down_step[None, :, :]
    stencil = -(upper_part + upper_part.transpose(0, 2, 1))
    identity = jnp.eye(P_SIZE, dtype=jnp.float32)
    spread = (noise_draw + noise_draw.transpose(0, 2, 1)) * (0.07071 * P_SIZE ** (-0.5))
    spread = spread * (1.0 - identity)[None, :, :]
    coupling = stencil + spread
    diagonal = jnp.sum(jnp.abs(coupling), axis=2) + margin
    return (coupling + identity[None, :, :] * diagonal[:, :, None]).astype(jnp.bfloat16)


def draw_separator(key, part):
    side = SEP
    rank_width = 2 * NB
    noise_key, margin_key, factor_key = jax.random.split(jax.random.fold_in(key, 11), 3)
    noise_draw = jax.random.normal(noise_key, (side, side), jnp.float32)
    margin = jax.random.uniform(margin_key, (side,), jnp.float32, 4.0, 6.0)
    factor = jax.random.normal(factor_key, (side, rank_width), jnp.float32) * (1.0 / rank_width) ** 0.5
    spread = (noise_draw + noise_draw.T) * (2.0 * 0.7071 / side)
    spread = spread * (1.0 - jnp.eye(side, dtype=jnp.float32))
    coupling = jnp.dot(factor, factor.T, precision=lax.Precision.HIGHEST)
    coupling = 0.5 * (coupling + coupling.T)
    matrix = spread + jnp.diag(jnp.sum(jnp.abs(spread), axis=1) + margin) + coupling
    return matrix.reshape(RL, N_ROW * NB, CL, N_COL * NB)


def draw_border_block(key, part):
    order_key, row_key, pair_key, level_key = jax.random.split(jax.random.fold_in(key, 37), 4)
    orders = jax.vmap(lambda single: jax.random.permutation(single, GROUPS))(jax.random.split(order_key, LEAVES))
    row_order = jax.vmap(lambda single: jax.random.permutation(single, N_ROW))(jax.random.split(row_key, LEAVES))
    stride = N_COL // N_ROW
    level_count = NBLK // N_COL
    pair_lift = jax.random.randint(pair_key, (LEAVES, N_ROW), 0, stride)
    level_lift = jax.random.randint(level_key, (LEAVES, N_COL), 0, level_count)
    row_class = orders % N_ROW
    col_class = orders % N_COL
    row_residue = jnp.take_along_axis(row_order, row_class, axis=1)
    pair_step = (orders // N_ROW + jnp.take_along_axis(pair_lift, row_class, axis=1)) % stride
    col_residue = row_residue + N_ROW * pair_step
    levels = (orders // N_COL + jnp.take_along_axis(level_lift, col_class, axis=1)) % level_count
    return (col_residue + N_COL * levels).astype(jnp.int32)


def with_ends(values, own_key, smallest, high):
    spot = [jax.random.randint(jax.random.fold_in(own_key, axis), (), 0, length) for axis, length in enumerate(values.shape)]
    main_axis = values.shape.index(max(values.shape))
    next_to = spot[:main_axis] + [(spot[main_axis] + 1) % values.shape[main_axis]] + spot[main_axis + 1:]
    return values.at[tuple(spot)].set(smallest).at[tuple(next_to)].set(high)


def shard_levels(rng, shape, pieces, low, high):
    gain = 1.0
    for dim, parts in pieces:
        draws = jax.random.uniform(jax.random.fold_in(jax.random.fold_in(rng, 6), dim), (parts,), jnp.float32, low / len(pieces), high / len(pieces))
        gain = gain * jnp.repeat(jnp.exp(draws), shape[dim] // parts).reshape((-1,) + (1,) * (len(shape) - 1 - dim))
    return gain


def normal_values(key, shape, scale, reach, cuts=(), kind=jnp.bfloat16):
    level = shard_levels(key, shape, cuts, -0.22, 0.18) if cuts else 1.0
    drawn = jax.random.normal(key, shape, jnp.float32) * scale * level
    return jnp.minimum(jnp.maximum(drawn, -reach), reach).astype(kind)


def setup_inputs(seed: int = 0) -> dict:
    arg_keys = jax.random.split(jax.random.key(seed), 8)
    return {
        "front_pivot": draw_front_pivot(jax.random.fold_in(arg_keys[7], 71), 0),
        "front_border": normal_values(arg_keys[1], (LEAVES, BORDER, P_SIZE), (4.0 * (RL * N_ROW) ** 0.5 * (P_SIZE * DEVICES * GROUPS) ** -0.5), 0.625, ((0, 512),)),
        "pivot_live": with_ends(jax.random.randint(arg_keys[2], (LEAVES,), P_SIZE // 2, P_SIZE + 1), jax.random.fold_in(arg_keys[2], 1), P_SIZE // 2, P_SIZE).astype(jnp.int32),
        "rows_live": with_ends(jax.random.randint(arg_keys[3], (LEAVES, GROUPS), NB // 2, NB + 1), jax.random.fold_in(arg_keys[3], 1), NB // 2, NB).astype(jnp.int32),
        "border_block": draw_border_block(jax.random.fold_in(arg_keys[7], 71), 0),
        "row_map": jax.vmap(lambda own: jax.random.permutation(own, NB))(jax.random.split(arg_keys[5], LEAVES * GROUPS)).reshape((LEAVES, GROUPS, NB)).astype(jnp.int32),
        "separator": draw_separator(jax.random.fold_in(arg_keys[7], 71), 0),
    }


highest = lax.Precision.HIGHEST

def leaf_tiles(pivot_front, border_front, pivot_count, row_counts, placement):
    pivot_width = pivot_front.shape[0]
    groups, block_size = placement.shape
    pivot_mask = (jnp.arange(pivot_width) < pivot_count).astype(jnp.float32)
    pivot_matrix = pivot_front.astype(jnp.float32) * pivot_mask[:, None] * pivot_mask[None, :] + jnp.diag(1.0 - pivot_mask)
    factor = jnp.linalg.cholesky(pivot_matrix)
    row_mask = (jnp.arange(block_size)[None, :] < row_counts[:, None]).astype(jnp.float32).reshape(groups * block_size)
    border = border_front.astype(jnp.float32) * row_mask[:, None] * pivot_mask[None, :]
    solved = jax.scipy.linalg.solve_triangular(factor, border.T, lower=True).T
    placing = (placement[:, None, :] == jnp.arange(block_size)[None, :, None]).astype(jnp.float32)
    placed = jnp.einsum('gik,gkp->gip', placing, solved.reshape(groups, block_size, pivot_width), precision=highest)
    return jnp.einsum('gip,hjp->ghij', placed, placed, precision=highest)

def reference(front_pivot, front_border, pivot_live, rows_live, border_block, row_map, separator):
    side = SEP

    def add_leaf(leaf_index, blocks_sum):
        tiles = leaf_tiles(front_pivot[leaf_index], front_border[leaf_index], pivot_live[leaf_index], rows_live[leaf_index], row_map[leaf_index])
        where_blocks = border_block[leaf_index]
        return blocks_sum.at[where_blocks[:, None], where_blocks[None, :]].add(tiles)
    summed = lax.fori_loop(0, LEAVES, add_leaf, jnp.zeros((NBLK, NBLK, NB, NB), jnp.float32))
    matrix = separator.reshape(side, side) - summed.transpose(0, 2, 1, 3).reshape(side, side)
    block_rows = jnp.arange(side) // NB
    for panel_index in range(PANELS):
        lower_edge = panel_index * NB
        pivot_factor = jnp.linalg.cholesky(matrix[lower_edge:lower_edge + NB, lower_edge:lower_edge + NB])
        solved = jax.scipy.linalg.solve_triangular(pivot_factor, matrix[:, lower_edge:lower_edge + NB].T, lower=True).T
        panel_part = jnp.where((block_rows > panel_index)[:, None], solved, 0.0)
        panel_part = panel_part.at[lower_edge:lower_edge + NB].set(pivot_factor)
        matrix = matrix - jnp.dot(panel_part, panel_part.T, precision=highest)
        matrix = matrix.at[:, lower_edge:lower_edge + NB].set(panel_part)
    return matrix.reshape(RL, N_ROW * NB, CL, N_COL * NB)
```

```python
import jax
import jax.numpy as jnp
from jax import lax
from jax.experimental import pallas as pl
from jax.experimental.pallas import tpu as pltpu
from jax.sharding import PartitionSpec as P

f32 = jnp.float32
highest = lax.Precision.HIGHEST
MESH = pl.DeviceIdType.MESH
NB = 128
GROUP = 128
ROWS = 16
SHARE = 1088
VMEM = pl.BlockSpec(memory_space=pltpu.VMEM)
SMEM = pl.BlockSpec(memory_space=pltpu.SMEM)


def dot_nt(a, b):
    return lax.dot_general(
        a, b, (((1,), (1,)), ((), ())), precision=highest, preferred_element_type=f32
    )


def dot_nn(a, b):
    return lax.dot_general(
        a, b, (((1,), (0,)), ((), ())), precision=highest, preferred_element_type=f32
    )


def factor_and_inverse(matrix):
    count = NB // 8
    lane = lax.broadcasted_iota(jnp.int32, (8, NB), 1)
    sub = lax.broadcasted_iota(jnp.int32, (8, NB), 0)
    left = [matrix[8 * i : 8 * i + 8, :] for i in range(count)]
    right = [jnp.where(lane == sub + 8 * i, 1.0, 0.0).astype(f32) for i in range(count)]
    for k in range(NB):
        t, s = divmod(k, 8)
        left_row = left[t][s : s + 1, :]
        right_row = right[t][s : s + 1, :]
        inverse = 1.0 / left_row[:, k : k + 1]
        left_row = left_row * inverse
        right_row = right_row * inverse
        for i in range(t, count):
            column = jnp.broadcast_to(left[i][:, k : k + 1], (8, NB))
            if i == t:
                column = jnp.where(sub > s, column, 0.0)
            left[i] = left[i] - column * left_row
            right[i] = right[i] - column * right_row
    for i in range(count):
        on_diagonal = lane == sub + 8 * i
        pivots = jnp.sum(jnp.where(on_diagonal, left[i], 0.0), axis=1, keepdims=True)
        scale = 1.0 / jnp.sqrt(pivots)
        left[i] = jnp.where(lane >= sub + 8 * i, left[i] * scale, 0.0)
        right[i] = right[i] * scale
    return jnp.concatenate(left, axis=0), jnp.concatenate(right, axis=0)


def leaf_kernel(live_ref, rows_ref, block_ref, map_ref, pivot_ref, border_ref, sep_ref, out_ref):
    live = live_ref[0]
    row = lax.broadcasted_iota(jnp.int32, (256, 256), 0)
    col = lax.broadcasted_iota(jnp.int32, (256, 256), 1)
    front = jnp.where(
        (row < live) & (col < live),
        pivot_ref[...].astype(f32),
        jnp.where(row == col, 1.0, 0.0),
    )
    first = factor_and_inverse(front[:NB, :NB])[1]
    below = dot_nt(front[NB:, :NB], first)
    second = factor_and_inverse(front[NB:, NB:] - dot_nt(below, below))[1]

    blocks = [block_ref[g] for g in range(4)]
    ranks = []
    for g in range(4):
        rank = jnp.int32(0)
        for h in range(4):
            if h != g:
                rank = rank + jnp.where(blocks[h] > blocks[g], 1, 0)
        ranks.append(rank)
    border_row = lax.broadcasted_iota(jnp.int32, (NB, 256), 0)
    border_col = lax.broadcasted_iota(jnp.int32, (NB, 256), 1)
    home = lax.broadcasted_iota(jnp.int32, (NB, NB), 0)
    borders, placings, labels = [], [], []
    for s in range(4):
        g = jnp.int32(0)
        for h in range(1, 4):
            g = jnp.where(ranks[h] == s, h, g)
        labels.append(block_ref[g])
        rows = border_ref[pl.ds(pl.multiple_of(g * NB, NB), NB), :].astype(f32)
        keep = (border_row < rows_ref[g]) & (border_col < live)
        borders.append(jnp.where(keep, rows, 0.0))
        placings.append(jnp.where(map_ref[pl.ds(g, 1), :] == home, 1.0, 0.0).astype(f32))
    border = jnp.concatenate(borders, axis=0)
    solved_first = dot_nt(border[:, :NB], first)
    solved_second = dot_nt(border[:, NB:] - dot_nt(solved_first, below), second)
    solved = jnp.concatenate([solved_first, solved_second], axis=1)
    placed = jnp.concatenate(
        [dot_nn(placings[s], solved[s * NB : s * NB + NB]) for s in range(4)], axis=0
    )
    slot = 0
    for s in range(4):
        tiles = dot_nt(placed[s * NB : s * NB + NB], placed[s * NB :])
        for t in range(4 - s):
            out_ref[pl.ds(slot, NB, stride=ROWS), :] = tiles[:, t * NB : t * NB + NB]
            slot += 1
    for k in range(2):
        out_ref[pl.ds(10 + k, NB, stride=ROWS), :] = sep_ref[k]
    lane = lax.broadcasted_iota(jnp.int32, (NB, NB), 1)
    label_row = jnp.zeros((NB, NB), jnp.int32)
    for s in range(4):
        label_row = jnp.where(lane == s, labels[s], label_row)
    out_ref[pl.ds(12, NB, stride=ROWS), :] = label_row.astype(f32)
    for k in range(13, ROWS):
        out_ref[pl.ds(k, NB, stride=ROWS), :] = jnp.zeros((NB, NB), f32)


def exchange_kernel(src_ref, dst_ref, send_sem, recv_sem, own_sem):
    layer = lax.axis_index("layer")
    row = lax.axis_index("row")
    col = lax.axis_index("col")
    high, core, depth, low = layer // 2, layer % 2, col // 2, col % 2
    me = high * 64 + row * 8 + depth

    def peer(step):
        to_high = (high + step // 64) % 2
        to_row = (row + (step // 8) % 8) % 8
        to_depth = (depth + step % 8) % 8
        where_to = (to_high * 2 + core, to_row, to_depth * 2 + low)
        return to_high * 64 + to_row * 8 + to_depth, where_to

    barrier = pltpu.get_barrier_semaphore()

    def greet(step, carry):
        pl.semaphore_signal(barrier, inc=1, device_id=peer(step)[1], device_id_type=MESH)
        return carry

    lax.fori_loop(1, GROUP, greet, 0)
    own = pltpu.make_async_copy(src_ref.at[me], dst_ref.at[me], own_sem)
    own.start()
    pl.semaphore_wait(barrier, GROUP - 1)

    def send(index, carry):
        step = (index * 37) % GROUP
        target, where_to = peer(step)
        pltpu.make_async_remote_copy(
            src_ref=src_ref.at[target],
            dst_ref=dst_ref.at[me],
            send_sem=send_sem,
            recv_sem=recv_sem,
            device_id=where_to,
            device_id_type=MESH,
        ).start()
        return carry

    lax.fori_loop(1, GROUP, send, 0)
    own.wait()
    everything = pltpu.make_async_remote_copy(
        src_ref=src_ref.at[pl.ds(0, GROUP - 1)],
        dst_ref=dst_ref.at[pl.ds(0, GROUP - 1)],
        send_sem=send_sem,
        recv_sem=recv_sem,
        device_id=peer(1)[1],
        device_id_type=MESH,
    )
    everything.wait_send()
    everything.wait_recv()


def exchange(array, collective_id):
    return pl.pallas_call(
        exchange_kernel,
        out_shape=jax.ShapeDtypeStruct((GROUP, ROWS, NB), f32),
        in_specs=[VMEM],
        out_specs=VMEM,
        scratch_shapes=[pltpu.SemaphoreType.DMA] * 3,
        compiler_params=pltpu.CompilerParams(collective_id=collective_id, has_side_effects=True),
        name="exchange",
    )(array)


def collect_kernel(row_ref, col_ref, side_ref, got_ref, out_ref):
    def clear(i, carry):
        out_ref[pl.ds(pl.multiple_of(i * 64, 64), 64), :] = jnp.zeros((64, NB), f32)
        return carry

    lax.fori_loop(0, 4 * SHARE // 64, clear, 0)

    def add(leaf, carry):
        rows = [row_ref[leaf * 4 + g] for g in range(4)]
        cols = [col_ref[leaf * 4 + g] for g in range(4)]
        places, values = [], []
        slot = 0
        for s in range(4):
            for t in range(s, 4):
                value = got_ref[pl.ds(leaf * ROWS + slot, 1), :]
                slot += 1
                places.append(rows[s] + cols[t])
                values.append(value)
                if t > s:
                    places.append(rows[t] + cols[s])
                    values.append(value)
        before = [out_ref[pl.ds(place, 1), :] for place in places]
        for place, old, value in zip(places, before, values):
            out_ref[pl.ds(place, 1), :] = old + value
        return carry

    lax.fori_loop(0, GROUP, add, 0)
    for block in range(64):
        layer, kk, row = block // 16, (block // 8) % 2, block % 8
        high, core = layer // 2, layer % 2
        at = core * SHARE + high * 512 + row * 64 + kk * 4
        mine = jnp.where((side_ref[0] == 0) & (side_ref[1] == core), 1.0, 0.0)
        given = got_ref[pl.ds((high * 64 + row * 8) * ROWS + 10 + kk, 1), :]
        panel_row = out_ref[pl.ds(at, 1), :] - given * mine
        for q in range(4):
            out_ref[pl.ds(q * SHARE + 1024 + block, 1), :] = panel_row


def join_kernel(src_ref, out_ref, near, cross, passing, total, send_sem, recv_sem):
    layer = lax.axis_index("layer")
    row = lax.axis_index("row")
    col = lax.axis_index("col")
    core, low = layer % 2, col % 2
    twin = (layer + 1 - 2 * core, row, col)
    beside = (layer, row, col + 1 - 2 * low)
    barrier = pltpu.get_barrier_semaphore()
    for other in (twin, beside):
        pl.semaphore_signal(barrier, inc=1, device_id=other, device_id_type=MESH)
    pl.semaphore_wait(barrier, 2)

    def copy(src, dst, index, other):
        return pltpu.make_async_remote_copy(
            src_ref=src,
            dst_ref=dst,
            send_sem=send_sem.at[index],
            recv_sem=recv_sem.at[index],
            device_id=other,
            device_id_type=MESH,
        )

    onward = copy(src_ref.at[(1 - low) * 2 + 1 - core], near.at[0], 0, twin)
    kept = copy(src_ref.at[low * 2 + 1 - core], near.at[1], 1, twin)
    onward.start()
    kept.start()
    onward.wait()
    passing[...] = src_ref[(1 - low) * 2 + core] + near[0]
    across = copy(passing, cross, 2, beside)
    across.start()
    kept.wait()
    total[...] = src_ref[low * 2 + core] + near[1]
    across.wait()
    total[...] = total[...] + cross[...]

    def lay_out(d, carry):
        to_high, to_row, to_depth = d // 64, (d // 8) % 8, d % 8
        out_ref[d, 0:8, :] = total[pl.ds(pl.multiple_of(d * 8, 8), 8), :]
        for kk in range(2):
            block = (to_high * 2 + core) * 16 + kk * 8 + to_row
            out_ref[d, 8 + kk : 9 + kk, :] = total[pl.ds(1024 + block, 1), :]
        for kc in range(4):
            block = kc * 16 + to_depth * 2 + low
            out_ref[d, 10 + kc : 11 + kc, :] = total[pl.ds(1024 + block, 1), :]
        out_ref[d, 14:15, :] = total[1024:1025, :]
        out_ref[d, 15:16, :] = total[1024:1025, :]
        return carry

    lax.fori_loop(0, GROUP, lay_out, 0)


def panel_kernel(place_ref, got_ref, sep_ref, out_ref):
    layer, row, col = place_ref[0], place_ref[1], place_ref[2]

    def tile(slot):
        return got_ref[pl.ds(slot, NB, stride=ROWS), :]

    upper, inverse = factor_and_inverse(-tile(14))
    lower = upper.T
    owned, crossing = [], []
    for kk in range(2):
        at_pivot = (2 * layer + kk) * 8 + row == 0
        owned.append(jnp.where(at_pivot, lower, dot_nt(-tile(8 + kk), inverse)))
    for kc in range(4):
        at_pivot = kc * 16 + col == 0
        crossing.append(jnp.where(at_pivot, lower, dot_nt(-tile(10 + kc), inverse)))
    for kk in range(2):
        for kc in range(4):
            update = tile(kk * 4 + kc)
            above = (2 * layer + kk) * 8 + row < kc * 16 + col
            update = jnp.where(above, update.T, update)
            product = dot_nt(owned[kk], crossing[kc])
            result = sep_ref[kk, pl.ds(kc, NB, stride=4), :] - update - product
            if kc == 0:
                result = jnp.where(col == 0, owned[kk], result)
            out_ref[kk, pl.ds(kc, NB, stride=4), :] = result


def shards(front_pivot, front_border, pivot_live, rows_live, border_block, row_map, separator):
    layer = lax.axis_index("layer")
    row = lax.axis_index("row")
    col = lax.axis_index("col")
    own_sep = lax.dynamic_slice_in_dim(separator, layer * 2, 2, 0)
    outgoing = pl.pallas_call(
        leaf_kernel,
        out_shape=jax.ShapeDtypeStruct((GROUP * ROWS, NB), f32),
        in_specs=[SMEM] * 3 + [VMEM] * 4,
        out_specs=VMEM,
        name="leaf",
    )(
        pivot_live,
        rows_live[0],
        border_block[0],
        row_map[0],
        front_pivot[0],
        front_border[0],
        own_sep[:, :, 0, :],
    )
    got = exchange(outgoing.reshape(GROUP, ROWS, NB), 0)
    blocks = got[:, 12, :4].astype(jnp.int32)
    level = blocks // 16
    row_at = (level % 2) * SHARE + (level // 2) * 512 + (blocks % 8) * 64 + (blocks // 8 % 2) * 4
    col_at = (blocks % 2) * (2 * SHARE) + (blocks % 16 // 2) * 8 + level
    side = jnp.stack([col % 2, layer % 2]).astype(jnp.int32)
    gathered = pl.pallas_call(
        collect_kernel,
        out_shape=jax.ShapeDtypeStruct((4 * SHARE, NB), f32),
        in_specs=[SMEM] * 3 + [VMEM],
        out_specs=VMEM,
        name="collect",
    )(row_at.reshape(-1), col_at.reshape(-1), side, got.reshape(GROUP * ROWS, NB))
    laid_out = pl.pallas_call(
        join_kernel,
        out_shape=jax.ShapeDtypeStruct((GROUP, ROWS, NB), f32),
        in_specs=[VMEM],
        out_specs=VMEM,
        scratch_shapes=[
            pltpu.VMEM((2, SHARE, NB), f32),
            pltpu.VMEM((SHARE, NB), f32),
            pltpu.VMEM((SHARE, NB), f32),
            pltpu.VMEM((SHARE, NB), f32),
            pltpu.SemaphoreType.DMA((3,)),
            pltpu.SemaphoreType.DMA((3,)),
        ],
        compiler_params=pltpu.CompilerParams(collective_id=1, has_side_effects=True),
        name="join",
    )(gathered.reshape(4, SHARE, NB))
    final = exchange(laid_out, 2)
    place = jnp.stack([layer, row, col]).astype(jnp.int32)
    result = pl.pallas_call(
        panel_kernel,
        out_shape=jax.ShapeDtypeStruct((2, 4 * NB, NB), f32),
        in_specs=[SMEM, VMEM, VMEM],
        out_specs=VMEM,
        name="panel",
    )(place, final.reshape(GROUP * ROWS, NB), own_sep.reshape(2, 4 * NB, NB))
    return result.reshape(2, NB, 4, NB)


def solution(mesh):
    placed = (
        P(("layer", "row", "col"), None, None),
        P(("layer", "row", "col"), None, None),
        P(("layer", "row", "col")),
        P(("layer", "row", "col"), None),
        P(("layer", "row", "col"), None),
        P(("layer", "row", "col"), None, None),
        P(None, "row", None, "col"),
    )
    return jax.shard_map(
        shards,
        mesh=mesh,
        in_specs=placed,
        out_specs=P("layer", "row", None, "col"),
        check_vma=False,
    )
```

```python
import jax
import jax.numpy as jnp
from jax import lax
from jax.experimental import pallas as pl
from jax.experimental.pallas import tpu as pltpu
from jax.sharding import PartitionSpec as P

f32 = jnp.float32
highest = lax.Precision.HIGHEST
MESH = pl.DeviceIdType.MESH
NB = 128
GROUP = 128
ROWS = 16
VMEM = pl.BlockSpec(memory_space=pltpu.VMEM)
SMEM = pl.BlockSpec(memory_space=pltpu.SMEM)


def dot_nt(a, b):
    return lax.dot_general(
        a, b, (((1,), (1,)), ((), ())), precision=highest, preferred_element_type=f32
    )


def dot_nn(a, b):
    return lax.dot_general(
        a, b, (((1,), (0,)), ((), ())), precision=highest, preferred_element_type=f32
    )


def factor_and_inverse(matrix):
    count = NB // 8
    lane = lax.broadcasted_iota(jnp.int32, (8, NB), 1)
    sub = lax.broadcasted_iota(jnp.int32, (8, NB), 0)

    def spread(block, s):
        return jnp.broadcast_to(block[s : s + 1, :], (8, NB))

    left = [matrix[8 * i : 8 * i + 8, :] for i in range(count)]
    right = [jnp.where(lane == sub + 8 * i, 1.0, 0.0).astype(f32) for i in range(count)]
    upper, inverse = [], []
    for t in range(count):
        columns = [
            [jnp.broadcast_to(left[i][:, 8 * t + s : 8 * t + s + 1], (8, NB)) for s in range(8)]
            for i in range(t, count)
        ]
        own = list(columns[0])
        rows, units = left[t], right[t]
        upper_rows, unit_rows, pivots = rows, units, own[0]
        for s in range(8):
            here = sub == s
            pivot = spread(own[s], s)
            scale = 1.0 / pivot
            row, unit = spread(rows, s), spread(units, s)
            upper_rows = jnp.where(here, row, upper_rows)
            unit_rows = jnp.where(here, unit, unit_rows)
            pivots = jnp.where(here, pivot, pivots)
            for j in range(s + 1, 8):
                ahead = spread(own[j], s) * scale
                own[j] = jnp.where(here, ahead, own[j] - own[s] * ahead)
            row, unit = row * scale, unit * scale
            rows = jnp.where(here, row, rows - own[s] * row)
            units = jnp.where(here, unit, units - own[s] * unit)
        for i in range(t + 1, count):
            for s in range(8):
                column = columns[i - t][s]
                left[i] = left[i] - column * spread(rows, s)
                right[i] = right[i] - column * spread(units, s)
        root = 1.0 / jnp.sqrt(pivots)
        upper.append(jnp.where(lane >= sub + 8 * t, upper_rows * root, 0.0))
        inverse.append(unit_rows * root)
    return jnp.concatenate(upper, axis=0), jnp.concatenate(inverse, axis=0)


class Peers:
    def __init__(self):
        self.layer = lax.axis_index("layer")
        self.row = lax.axis_index("row")
        self.col = lax.axis_index("col")
        self.high, self.core = self.layer // 2, lax.rem(self.layer, 2)
        self.depth, self.low = self.col // 2, lax.rem(self.col, 2)
        self.depths = [lax.rem(self.depth + dz, 8) for dz in range(8)]
        self.me = self.high * 64 + self.row * 8 + self.depth

    def at(self, dx, dy, dz):
        to_high = self.high if dx == 0 else 1 - self.high
        to_row = lax.rem(self.row + dy, 8)
        to_depth = self.depths[dz]
        place = (to_high * 2 + self.core, to_row, to_depth * 2 + self.low)
        return to_high * 64 + to_row * 8 + to_depth, place

    def visit(self, act, steps=range(8)):
        for dz in steps:
            if dz:
                act(*self.at(0, 0, dz))

        def near(dy, carry):
            for dz in steps:
                act(*self.at(0, dy, dz))
            return carry

        def far(dy, carry):
            for dz in steps:
                act(*self.at(1, dy, dz))
            return carry

        lax.fori_loop(1, 8, near, 0)
        lax.fori_loop(0, 8, far, 0)


def remote(src, dst, send_sem, recv_sem, place):
    return pltpu.make_async_remote_copy(
        src_ref=src,
        dst_ref=dst,
        send_sem=send_sem,
        recv_sem=recv_sem,
        device_id=place,
        device_id_type=MESH,
    )


def leaf_kernel(
    live_ref, rows_ref, block_ref, map_ref, pivot_ref, border_ref, sep_ref,
    got_ref, side_ref, out, early, send_sem, recv_sem, own_sem,
):
    peers = Peers()
    barrier = pltpu.get_barrier_semaphore()

    def greet(target, place):
        pl.semaphore_signal(barrier, inc=1, device_id=place, device_id_type=MESH)

    peers.visit(greet)

    blocks = [block_ref[g] for g in range(4)]
    ranks = []
    for g in range(4):
        rank = jnp.int32(0)
        for h in range(4):
            if h != g:
                rank = rank + jnp.where(blocks[h] > blocks[g], 1, 0)
        ranks.append(rank)
    order, labels = [], []
    for s in range(4):
        g, b = jnp.int32(0), blocks[0]
        for h in range(1, 4):
            g = jnp.where(ranks[h] == s, h, g)
            b = jnp.where(ranks[h] == s, blocks[h], b)
        order.append(g)
        labels.append(b)
    lane = lax.broadcasted_iota(jnp.int32, (NB, NB), 1)
    where_row = jnp.zeros((NB, NB), jnp.int32)
    for s in range(4):
        b = labels[s]
        level = b // 16
        row_at = (level % 2) * 1024 + (level // 2) * 512 + (b % 8) * 64 + (b // 8 % 2) * 4
        col_at = (b % 2) * 2048 + (b % 16 // 2) * 8 + level
        where_row = jnp.where(lane == s, row_at, where_row)
        where_row = jnp.where(lane == 4 + s, col_at, where_row)
    early_rows = early.reshape(GROUP * 8, NB)
    for k in range(2):
        early_rows[pl.ds(k, NB, stride=8), :] = sep_ref[k]
    early_rows[pl.ds(2, NB, stride=8), :] = where_row.astype(f32)

    live = live_ref[0]
    row = lax.broadcasted_iota(jnp.int32, (256, 256), 0)
    col = lax.broadcasted_iota(jnp.int32, (256, 256), 1)
    front = jnp.where(
        (row < live) & (col < live),
        pivot_ref[...].astype(f32),
        jnp.where(row == col, 1.0, 0.0),
    )
    first = factor_and_inverse(front[:NB, :NB])[1]

    pl.semaphore_wait(barrier, GROUP - 1)
    own_side = pltpu.make_async_copy(
        early.at[peers.me, pl.ds(0, 3)], side_ref.at[peers.me, pl.ds(0, 3)], own_sem.at[0]
    )
    own_side.start()

    def send_early(target, place):
        remote(
            early.at[target, pl.ds(0, 3)],
            side_ref.at[peers.me, pl.ds(0, 3)],
            send_sem.at[0],
            recv_sem.at[0],
            place,
        ).start()

    peers.visit(send_early)

    below = dot_nt(front[NB:, :NB], first)
    second = factor_and_inverse(front[NB:, NB:] - dot_nt(below, below))[1]
    border_row = lax.broadcasted_iota(jnp.int32, (NB, 256), 0)
    border_col = lax.broadcasted_iota(jnp.int32, (NB, 256), 1)
    home = lax.broadcasted_iota(jnp.int32, (NB, NB), 0)
    borders, placings = [], []
    for g in range(4):
        rows = border_ref[g * NB : g * NB + NB, :].astype(f32)
        keep = (border_row < rows_ref[g]) & (border_col < live)
        borders.append(jnp.where(keep, rows, 0.0))
        placings.append(jnp.where(map_ref[g : g + 1, :] == home, 1.0, 0.0).astype(f32))
    border = jnp.concatenate(borders, axis=0)
    solved_first = dot_nt(border[:, :NB], first)
    solved_second = dot_nt(border[:, NB:] - dot_nt(solved_first, below), second)
    solved = jnp.concatenate([solved_first, solved_second], axis=1)
    by_group = [dot_nn(placings[g], solved[g * NB : g * NB + NB]) for g in range(4)]
    in_order = []
    for s in range(4):
        chosen = by_group[0]
        for g in range(1, 4):
            chosen = jnp.where(order[s] == g, by_group[g], chosen)
        in_order.append(chosen)
    placed = jnp.concatenate(in_order, axis=0)
    out_rows = out.reshape(GROUP * ROWS, NB)
    slot = 0
    for s in range(4):
        tiles = dot_nt(placed[s * NB : s * NB + NB], placed[s * NB :])
        for t in range(4 - s):
            out_rows[pl.ds(slot, NB, stride=ROWS), :] = tiles[:, t * NB : t * NB + NB]
            slot += 1
    own_tiles = pltpu.make_async_copy(
        out.at[peers.me, pl.ds(0, 10)], got_ref.at[peers.me, pl.ds(0, 10)], own_sem.at[1]
    )
    own_tiles.start()

    def send_tiles(target, place):
        remote(
            out.at[target, pl.ds(0, 10)],
            got_ref.at[peers.me, pl.ds(0, 10)],
            send_sem.at[1],
            recv_sem.at[1],
            place,
        ).start()

    peers.visit(send_tiles)
    own_side.wait()
    own_tiles.wait()
    for index, src, dst, size in ((0, early, side_ref, 3), (1, out, got_ref, 10)):
        everything = remote(
            src.at[pl.ds(0, GROUP - 1), pl.ds(0, size)],
            dst.at[pl.ds(0, GROUP - 1), pl.ds(0, size)],
            send_sem.at[index],
            recv_sem.at[index],
            peers.at(0, 0, 1)[1],
        )
        everything.wait_send()
        everything.wait_recv()


def collect_kernel(where_ref, got_ref, side_ref, out_ref, panel_ref):
    core_here = lax.rem(lax.axis_index("layer"), 2)
    low = lax.rem(lax.axis_index("col"), 2)

    def clear(i, carry):
        out_ref[pl.ds(pl.multiple_of(i * 128, 128), 128), :] = jnp.zeros((128, NB), f32)
        return carry

    lax.fori_loop(0, 32, clear, 0)

    def add(leaf, carry):
        rows = [where_ref[leaf * 8 + g] for g in range(4)]
        cols = [where_ref[leaf * 8 + 4 + g] for g in range(4)]
        places, values = [], []
        slot = 0
        for s in range(4):
            for t in range(s, 4):
                value = got_ref[pl.ds(leaf * ROWS + slot, 1), :]
                slot += 1
                places.append(rows[s] + cols[t])
                values.append(value)
                if t > s:
                    places.append(rows[t] + cols[s])
                    values.append(value)
        before = [out_ref[pl.ds(place, 1), :] for place in places]
        for place, old, value in zip(places, before, values):
            out_ref[pl.ds(place, 1), :] = old + value
        return carry

    lax.fori_loop(0, GROUP, add, 0)
    for block in range(64):
        layer, kk, row = block // 16, (block // 8) % 2, block % 8
        high, core = layer // 2, layer % 2
        at = core * 1024 + high * 512 + row * 64 + kk * 4
        mine = jnp.where((low == 0) & (core_here == core), 1.0, 0.0)
        given = side_ref[pl.ds((high * 64 + row * 8) * 8 + kk, 1), :]
        panel_ref[pl.ds(block, 1), :] = out_ref[pl.ds(at, 1), :] - given * mine


def finish_kernel(
    src_ref, panel_ref, sep_ref, out_ref, near, cross, passing, total, joined, others, fan,
    got, extra, twin_send, twin_recv, cross_send, cross_recv, panel_send, panel_recv,
    send_sem, recv_sem, own_sem,
):
    peers = Peers()
    layer, row, col = peers.layer, peers.row, peers.col
    core, low, me = peers.core, peers.low, peers.me
    twin = (layer + 1 - 2 * core, row, col)
    beside = (layer, row, col + 1 - 2 * low)
    opposite = (layer + 1 - 2 * core, row, col + 1 - 2 * low)
    barrier = pltpu.get_barrier_semaphore()

    def greet(target, place):
        pl.semaphore_signal(barrier, inc=1, device_id=place, device_id_type=MESH)

    for place in (twin, beside, opposite):
        greet(0, place)
    peers.visit(greet)
    pl.semaphore_wait(barrier, GROUP + 2)

    panels = []
    for index, place in enumerate((twin, beside, opposite)):
        panels.append(
            remote(panel_ref, others.at[index], panel_send.at[index], panel_recv.at[index], place)
        )
    onward = remote(
        src_ref.at[(1 - low) * 2 + 1 - core], near.at[0], twin_send.at[0], twin_recv.at[0], twin
    )
    kept = remote(
        src_ref.at[low * 2 + 1 - core], near.at[1], twin_send.at[1], twin_recv.at[1], twin
    )
    for copy in (*panels, onward, kept):
        copy.start()

    onward.wait()
    across = []
    for dz in range(8):
        piece = pl.ds(pl.multiple_of(peers.depths[dz] * 8, 8), 8)
        passing[:, piece, :] = src_ref[(1 - low) * 2 + core, :, piece, :] + near[0, :, piece, :]
        across.append(
            remote(
                passing.at[:, piece],
                cross.at[:, piece],
                cross_send.at[dz],
                cross_recv.at[dz],
                beside,
            )
        )
        if dz < 2:
            across[dz].start()

    for copy in panels:
        copy.wait()
    joined[...] = panel_ref[...] + others[0] + others[1] + others[2]

    def lay_out(d, carry):
        to_high, to_row, to_depth = d // 64, lax.rem(d // 8, 8), lax.rem(d, 8)
        for kk in range(2):
            block = (to_high * 2 + core) * 16 + kk * 8 + to_row
            fan[d, kk : kk + 1, :] = joined[pl.ds(block, 1), :]
        for kc in range(4):
            block = kc * 16 + to_depth * 2 + low
            fan[d, 2 + kc : 3 + kc, :] = joined[pl.ds(block, 1), :]
        fan[d, 6:7, :] = joined[0:1, :]
        return carry

    lax.fori_loop(0, GROUP, lay_out, 0)
    own_extra = pltpu.make_async_copy(
        fan.at[me, pl.ds(0, 7)], extra.at[me, pl.ds(0, 7)], own_sem.at[0]
    )
    own_extra.start()

    def send_extra(target, place):
        remote(
            fan.at[target, pl.ds(0, 7)],
            extra.at[me, pl.ds(0, 7)],
            send_sem.at[0],
            recv_sem.at[0],
            place,
        ).start()

    peers.visit(send_extra)
    for dz in range(2, 8):
        across[dz].start()
    kept.wait()
    own_rows = None
    for dz in range(8):
        piece = pl.ds(pl.multiple_of(peers.depths[dz] * 8, 8), 8)
        across[dz].wait()
        total[:, piece, :] = (
            src_ref[low * 2 + core, :, piece, :] + near[1, :, piece, :] + cross[:, piece, :]
        )
        if dz == 0:
            own_rows = pltpu.make_async_copy(
                total.at[peers.high * 8 + row, piece], got.at[me], own_sem.at[1]
            )
            own_rows.start()

        def send_rows(target, place, piece=piece):
            remote(
                total.at[target // 8, piece], got.at[me], send_sem.at[1], recv_sem.at[1], place
            ).start()

        peers.visit(send_rows, (dz,))

    def arrived(index, src, dst, size):
        everything = remote(
            src.at[pl.ds(0, GROUP - 1), pl.ds(0, size)],
            dst.at[pl.ds(0, GROUP - 1), pl.ds(0, size)],
            send_sem.at[index],
            recv_sem.at[index],
            peers.at(0, 0, 1)[1],
        )
        everything.wait_send()
        everything.wait_recv()

    own_extra.wait()
    arrived(0, fan, extra, 7)
    extra_rows = extra.reshape(GROUP * 8, NB)
    got_rows = got.reshape(GROUP * 8, NB)

    def panel_tile(slot):
        return -extra_rows[pl.ds(slot, NB, stride=8), :]

    upper, inverse = factor_and_inverse(panel_tile(6))
    lower = upper.T
    owned, crossing = [], []
    for kk in range(2):
        at_pivot = (2 * layer + kk) * 8 + row == 0
        owned.append(jnp.where(at_pivot, lower, dot_nt(panel_tile(kk), inverse)))
    for kc in range(4):
        at_pivot = kc * 16 + col == 0
        crossing.append(jnp.where(at_pivot, lower, dot_nt(panel_tile(2 + kc), inverse)))
    for kk in range(2):
        for kc in range(4):
            product = dot_nt(owned[kk], crossing[kc])
            out_ref[kk, pl.ds(kc, NB, stride=4), :] = (
                sep_ref[kk, pl.ds(kc, NB, stride=4), :] - product
            )
    own_rows.wait()
    arrived(1, got, got, 8)
    for kk in range(2):
        for kc in range(4):
            update = got_rows[pl.ds(kk * 4 + kc, NB, stride=8), :]
            above = (2 * layer + kk) * 8 + row < kc * 16 + col
            update = jnp.where(above, update.T, update)
            result = out_ref[kk, pl.ds(kc, NB, stride=4), :] - update
            if kc == 0:
                result = jnp.where(col == 0, owned[kk], result)
            out_ref[kk, pl.ds(kc, NB, stride=4), :] = result


def shards(front_pivot, front_border, pivot_live, rows_live, border_block, row_map, separator):
    layer = lax.axis_index("layer")
    own_sep = lax.dynamic_slice_in_dim(separator, layer * 2, 2, 0)
    dma = pltpu.SemaphoreType.DMA
    got, side = pl.pallas_call(
        leaf_kernel,
        out_shape=[
            jax.ShapeDtypeStruct((GROUP, ROWS, NB), f32),
            jax.ShapeDtypeStruct((GROUP, 8, NB), f32),
        ],
        in_specs=[SMEM] * 3 + [VMEM] * 4,
        out_specs=[VMEM, VMEM],
        scratch_shapes=[
            pltpu.VMEM((GROUP, ROWS, NB), f32),
            pltpu.VMEM((GROUP, 8, NB), f32),
            dma((2,)),
            dma((2,)),
            dma((2,)),
        ],
        compiler_params=pltpu.CompilerParams(collective_id=0, has_side_effects=True),
        name="leaf",
    )(
        pivot_live,
        rows_live[0],
        border_block[0],
        row_map[0],
        front_pivot[0],
        front_border[0],
        own_sep[:, :, 0, :],
    )
    places = side[:, 2, :8].astype(jnp.int32).reshape(GROUP * 8)
    gathered, panel = pl.pallas_call(
        collect_kernel,
        out_shape=[
            jax.ShapeDtypeStruct((4 * 1024, NB), f32),
            jax.ShapeDtypeStruct((64, NB), f32),
        ],
        in_specs=[SMEM, VMEM, VMEM],
        out_specs=[VMEM, VMEM],
        name="collect",
    )(places, got.reshape(GROUP * ROWS, NB), side.reshape(GROUP * 8, NB))
    result = pl.pallas_call(
        finish_kernel,
        out_shape=jax.ShapeDtypeStruct((2, 4 * NB, NB), f32),
        in_specs=[VMEM] * 3,
        out_specs=VMEM,
        scratch_shapes=[
            pltpu.VMEM((2, 16, 64, NB), f32),
            pltpu.VMEM((16, 64, NB), f32),
            pltpu.VMEM((16, 64, NB), f32),
            pltpu.VMEM((16, 64, NB), f32),
            pltpu.VMEM((64, NB), f32),
            pltpu.VMEM((3, 64, NB), f32),
            pltpu.VMEM((GROUP, 8, NB), f32),
            pltpu.VMEM((GROUP, 8, NB), f32),
            pltpu.VMEM((GROUP, 8, NB), f32),
            dma((2,)),
            dma((2,)),
            dma((8,)),
            dma((8,)),
            dma((3,)),
            dma((3,)),
            dma((2,)),
            dma((2,)),
            dma((2,)),
        ],
        compiler_params=pltpu.CompilerParams(collective_id=1, has_side_effects=True),
        name="finish",
    )(gathered.reshape(4, 16, 64, NB), panel, own_sep.reshape(2, 4 * NB, NB))
    return result.reshape(2, NB, 4, NB)


def solution(mesh):
    placed = (
        P(("layer", "row", "col"), None, None),
        P(("layer", "row", "col"), None, None),
        P(("layer", "row", "col")),
        P(("layer", "row", "col"), None),
        P(("layer", "row", "col"), None),
        P(("layer", "row", "col"), None, None),
        P(None, "row", None, "col"),
    )
    return jax.shard_map(
        shards,
        mesh=mesh,
        in_specs=placed,
        out_specs=P("layer", "row", None, "col"),
        check_vma=False,
    )
```

```python
import jax
import jax.numpy as jnp
from jax import lax
from jax.experimental import pallas as pl
from jax.experimental.pallas import tpu as pltpu
from jax.sharding import PartitionSpec as P

f32 = jnp.float32
highest = lax.Precision.HIGHEST
MESH = pl.DeviceIdType.MESH
NB = 128
GROUP = 128
ROWS = 16
VMEM = pl.BlockSpec(memory_space=pltpu.VMEM)
SMEM = pl.BlockSpec(memory_space=pltpu.SMEM)
ANY = pl.BlockSpec(memory_space=pl.ANY)


def dot_nt(a, b):
    return lax.dot_general(
        a, b, (((1,), (1,)), ((), ())), precision=highest, preferred_element_type=f32
    )


def dot_nn(a, b):
    return lax.dot_general(
        a, b, (((1,), (0,)), ((), ())), precision=highest, preferred_element_type=f32
    )


def factor_and_inverse(matrix):
    count = NB // 8
    lane = lax.broadcasted_iota(jnp.int32, (8, NB), 1)
    sub = lax.broadcasted_iota(jnp.int32, (8, NB), 0)

    def spread(block, s):
        return jnp.broadcast_to(block[s : s + 1, :], (8, NB))

    left = [matrix[8 * i : 8 * i + 8, :] for i in range(count)]
    right = [jnp.where(lane == sub + 8 * i, 1.0, 0.0).astype(f32) for i in range(count)]
    upper, inverse = [], []
    for t in range(count):
        columns = [
            [jnp.broadcast_to(left[i][:, 8 * t + s : 8 * t + s + 1], (8, NB)) for s in range(8)]
            for i in range(t, count)
        ]
        own = list(columns[0])
        rows, units = left[t], right[t]
        upper_rows, unit_rows, pivots = rows, units, own[0]
        for s in range(8):
            here = sub == s
            pivot = spread(own[s], s)
            scale = 1.0 / pivot
            row, unit = spread(rows, s), spread(units, s)
            upper_rows = jnp.where(here, row, upper_rows)
            unit_rows = jnp.where(here, unit, unit_rows)
            pivots = jnp.where(here, pivot, pivots)
            for j in range(s + 1, 8):
                ahead = spread(own[j], s) * scale
                own[j] = jnp.where(here, ahead, own[j] - own[s] * ahead)
            row, unit = row * scale, unit * scale
            rows = jnp.where(here, row, rows - own[s] * row)
            units = jnp.where(here, unit, units - own[s] * unit)
        for i in range(t + 1, count):
            for s in range(8):
                column = columns[i - t][s]
                left[i] = left[i] - column * spread(rows, s)
                right[i] = right[i] - column * spread(units, s)
        root = 1.0 / jnp.sqrt(pivots)
        upper.append(jnp.where(lane >= sub + 8 * t, upper_rows * root, 0.0))
        inverse.append(unit_rows * root)
    return jnp.concatenate(upper, axis=0), jnp.concatenate(inverse, axis=0)


class Peers:
    def __init__(self):
        self.layer = lax.axis_index("layer")
        self.row = lax.axis_index("row")
        self.col = lax.axis_index("col")
        self.high, self.core = self.layer // 2, lax.rem(self.layer, 2)
        self.depth, self.low = self.col // 2, lax.rem(self.col, 2)
        self.depths = [lax.rem(self.depth + dz, 8) for dz in range(8)]
        self.me = self.high * 64 + self.row * 8 + self.depth

    def at(self, dx, dy, dz):
        to_high = self.high if dx == 0 else 1 - self.high
        to_row = lax.rem(self.row + dy, 8)
        to_depth = self.depths[dz]
        place = (to_high * 2 + self.core, to_row, to_depth * 2 + self.low)
        return to_high * 64 + to_row * 8 + to_depth, place

    def visit(self, act, steps=range(8)):
        for dz in steps:
            if dz:
                act(*self.at(0, 0, dz))

        def near(dy, carry):
            for dz in steps:
                act(*self.at(0, dy, dz))
            return carry

        def far(dy, carry):
            for dz in steps:
                act(*self.at(1, dy, dz))
            return carry

        lax.fori_loop(1, 8, near, 0)
        lax.fori_loop(0, 8, far, 0)


def remote(src, dst, send_sem, recv_sem, place):
    return pltpu.make_async_remote_copy(
        src_ref=src,
        dst_ref=dst,
        send_sem=send_sem,
        recv_sem=recv_sem,
        device_id=place,
        device_id_type=MESH,
    )


def leaf_kernel(
    live_ref, rows_ref, block_ref, map_ref, pivot_ref, border_ref, sep_ref,
    got_ref, side_ref, out, early, column, send_sem, recv_sem, own_sem, column_sem,
):
    peers = Peers()
    fetch = pltpu.make_async_copy(
        sep_ref.at[pl.ds(peers.layer * 2, 2), :, 0, :], column, column_sem
    )
    fetch.start()
    barrier = pltpu.get_barrier_semaphore()

    def greet(target, place):
        pl.semaphore_signal(barrier, inc=1, device_id=place, device_id_type=MESH)

    peers.visit(greet)

    blocks = [block_ref[g] for g in range(4)]
    ranks = []
    for g in range(4):
        rank = jnp.int32(0)
        for h in range(4):
            if h != g:
                rank = rank + jnp.where(blocks[h] > blocks[g], 1, 0)
        ranks.append(rank)
    order, labels = [], []
    for s in range(4):
        g, b = jnp.int32(0), blocks[0]
        for h in range(1, 4):
            g = jnp.where(ranks[h] == s, h, g)
            b = jnp.where(ranks[h] == s, blocks[h], b)
        order.append(g)
        labels.append(b)
    lane = lax.broadcasted_iota(jnp.int32, (NB, NB), 1)
    where_row = jnp.zeros((NB, NB), jnp.int32)
    for s in range(4):
        b = labels[s]
        level = b // 16
        row_at = (level % 2) * 1024 + (level // 2) * 512 + (b % 8) * 64 + (b // 8 % 2) * 4
        col_at = (b % 2) * 2048 + (b % 16 // 2) * 8 + level
        where_row = jnp.where(lane == s, row_at, where_row)
        where_row = jnp.where(lane == 4 + s, col_at, where_row)
    early_rows = early.reshape(GROUP * 8, NB)
    early_rows[pl.ds(2, NB, stride=8), :] = where_row.astype(f32)

    live = live_ref[0]
    row = lax.broadcasted_iota(jnp.int32, (256, 256), 0)
    col = lax.broadcasted_iota(jnp.int32, (256, 256), 1)
    front = jnp.where(
        (row < live) & (col < live),
        pivot_ref[...].astype(f32),
        jnp.where(row == col, 1.0, 0.0),
    )
    first = factor_and_inverse(front[:NB, :NB])[1]

    fetch.wait()
    for k in range(2):
        early_rows[pl.ds(k, NB, stride=8), :] = column[k]
    pl.semaphore_wait(barrier, GROUP - 1)
    own_side = pltpu.make_async_copy(
        early.at[peers.me, pl.ds(0, 3)], side_ref.at[peers.me, pl.ds(0, 3)], own_sem.at[0]
    )
    own_side.start()

    def send_early(target, place):
        remote(
            early.at[target, pl.ds(0, 3)],
            side_ref.at[peers.me, pl.ds(0, 3)],
            send_sem.at[0],
            recv_sem.at[0],
            place,
        ).start()

    peers.visit(send_early)

    below = dot_nt(front[NB:, :NB], first)
    second = factor_and_inverse(front[NB:, NB:] - dot_nt(below, below))[1]
    border_row = lax.broadcasted_iota(jnp.int32, (NB, 256), 0)
    border_col = lax.broadcasted_iota(jnp.int32, (NB, 256), 1)
    home = lax.broadcasted_iota(jnp.int32, (NB, NB), 0)
    borders, placings = [], []
    for g in range(4):
        rows = border_ref[g * NB : g * NB + NB, :].astype(f32)
        keep = (border_row < rows_ref[g]) & (border_col < live)
        borders.append(jnp.where(keep, rows, 0.0))
        placings.append(jnp.where(map_ref[g : g + 1, :] == home, 1.0, 0.0).astype(f32))
    border = jnp.concatenate(borders, axis=0)
    solved_first = dot_nt(border[:, :NB], first)
    solved_second = dot_nt(border[:, NB:] - dot_nt(solved_first, below), second)
    solved = jnp.concatenate([solved_first, solved_second], axis=1)
    by_group = [dot_nn(placings[g], solved[g * NB : g * NB + NB]) for g in range(4)]
    in_order = []
    for s in range(4):
        chosen = by_group[0]
        for g in range(1, 4):
            chosen = jnp.where(order[s] == g, by_group[g], chosen)
        in_order.append(chosen)
    placed = jnp.concatenate(in_order, axis=0)
    out_rows = out.reshape(GROUP * ROWS, NB)
    slot = 0
    for s in range(4):
        tiles = dot_nt(placed[s * NB : s * NB + NB], placed[s * NB :])
        for t in range(4 - s):
            out_rows[pl.ds(slot, NB, stride=ROWS), :] = tiles[:, t * NB : t * NB + NB]
            slot += 1
    own_tiles = pltpu.make_async_copy(
        out.at[peers.me, pl.ds(0, 10)], got_ref.at[peers.me, pl.ds(0, 10)], own_sem.at[1]
    )
    own_tiles.start()

    def send_tiles(target, place):
        remote(
            out.at[target, pl.ds(0, 10)],
            got_ref.at[peers.me, pl.ds(0, 10)],
            send_sem.at[1],
            recv_sem.at[1],
            place,
        ).start()

    peers.visit(send_tiles)
    own_side.wait()
    own_tiles.wait()
    for index, src, dst, size in ((0, early, side_ref, 3), (1, out, got_ref, 10)):
        everything = remote(
            src.at[pl.ds(0, GROUP - 1), pl.ds(0, size)],
            dst.at[pl.ds(0, GROUP - 1), pl.ds(0, size)],
            send_sem.at[index],
            recv_sem.at[index],
            peers.at(0, 0, 1)[1],
        )
        everything.wait_send()
        everything.wait_recv()


def collect_kernel(got_ref, side_ref, out_ref, panel_ref, where_at, column, sems):
    get_places = pltpu.make_async_copy(side_ref.at[:, :, 2, :], where_at, sems.at[0])
    get_column = pltpu.make_async_copy(side_ref.at[:, 0], column, sems.at[1])
    get_places.start()
    get_column.start()
    core_here = lax.rem(lax.axis_index("layer"), 2)
    low = lax.rem(lax.axis_index("col"), 2)

    def clear(i, carry):
        out_ref[pl.ds(pl.multiple_of(i * 128, 128), 128), :] = jnp.zeros((128, NB), f32)
        return carry

    lax.fori_loop(0, 32, clear, 0)
    get_places.wait()
    get_column.wait()

    def add(leaf, carry):
        high, low_part = leaf // 8, lax.rem(leaf, 8)
        rows = [where_at[high, low_part, g].astype(jnp.int32) for g in range(4)]
        cols = [where_at[high, low_part, 4 + g].astype(jnp.int32) for g in range(4)]
        places, values = [], []
        slot = 0
        for s in range(4):
            for t in range(s, 4):
                value = got_ref[pl.ds(leaf * ROWS + slot, 1), :]
                slot += 1
                places.append(rows[s] + cols[t])
                values.append(value)
                if t > s:
                    places.append(rows[t] + cols[s])
                    values.append(value)
        before = [out_ref[pl.ds(place, 1), :] for place in places]
        for place, old, value in zip(places, before, values):
            out_ref[pl.ds(place, 1), :] = old + value
        return carry

    lax.fori_loop(0, GROUP, add, 0)
    for block in range(64):
        layer, kk, row = block // 16, (block // 8) % 2, block % 8
        high, core = layer // 2, layer % 2
        at = core * 1024 + high * 512 + row * 64 + kk * 4
        mine = jnp.where((low == 0) & (core_here == core), 1.0, 0.0)
        given = column[high * 8 + row, kk : kk + 1, :]
        panel_ref[pl.ds(block, 1), :] = out_ref[pl.ds(at, 1), :] - given * mine


def finish_kernel(
    src_ref, panel_ref, sep_ref, out_ref, held, corner, near, cross, passing, total, joined, others, fan,
    got, extra, twin_send, twin_recv, cross_send, cross_recv, panel_send, panel_recv,
    send_sem, recv_sem, own_sem, load_sem,
):
    peers = Peers()
    loads = [
        pltpu.make_async_copy(
            src_ref.at[q * 2 + peers.core], held.at[q], load_sem.at[q]
        )
        for q in range(2)
    ]
    loads.append(
        pltpu.make_async_copy(sep_ref.at[pl.ds(peers.layer * 2, 2)], corner, load_sem.at[2])
    )
    for load in loads:
        load.start()
    layer, row, col = peers.layer, peers.row, peers.col
    core, low, me = peers.core, peers.low, peers.me
    twin = (layer + 1 - 2 * core, row, col)
    beside = (layer, row, col + 1 - 2 * low)
    opposite = (layer + 1 - 2 * core, row, col + 1 - 2 * low)
    barrier = pltpu.get_barrier_semaphore()

    def greet(target, place):
        pl.semaphore_signal(barrier, inc=1, device_id=place, device_id_type=MESH)

    for place in (twin, beside, opposite):
        greet(0, place)
    peers.visit(greet)
    pl.semaphore_wait(barrier, GROUP + 2)

    panels = []
    for index, place in enumerate((twin, beside, opposite)):
        panels.append(
            remote(panel_ref, others.at[index], panel_send.at[index], panel_recv.at[index], place)
        )
    onward = remote(
        src_ref.at[(1 - low) * 2 + 1 - core], near.at[0], twin_send.at[0], twin_recv.at[0], twin
    )
    kept = remote(
        src_ref.at[low * 2 + 1 - core], near.at[1], twin_send.at[1], twin_recv.at[1], twin
    )
    for copy in (*panels, onward, kept):
        copy.start()

    for load in loads:
        load.wait()
    onward.wait()
    across = []
    for dz in range(8):
        piece = pl.ds(pl.multiple_of(peers.depths[dz] * 8, 8), 8)
        passing[:, piece, :] = held[1 - low, :, piece, :] + near[0, :, piece, :]
        across.append(
            remote(
                passing.at[:, piece],
                cross.at[:, piece],
                cross_send.at[dz],
                cross_recv.at[dz],
                beside,
            )
        )
        across[dz].start()

    for copy in panels:
        copy.wait()
    joined[...] = panel_ref[...] + others[0] + others[1] + others[2]

    def lay_out(d, carry):
        to_high, to_row, to_depth = d // 64, lax.rem(d // 8, 8), lax.rem(d, 8)
        for kk in range(2):
            block = (to_high * 2 + core) * 16 + kk * 8 + to_row
            fan[d, kk : kk + 1, :] = joined[pl.ds(block, 1), :]
        for kc in range(4):
            block = kc * 16 + to_depth * 2 + low
            fan[d, 2 + kc : 3 + kc, :] = joined[pl.ds(block, 1), :]
        fan[d, 6:7, :] = joined[0:1, :]
        return carry

    lax.fori_loop(0, GROUP, lay_out, 0)
    own_extra = pltpu.make_async_copy(
        fan.at[me, pl.ds(0, 7)], extra.at[me, pl.ds(0, 7)], own_sem.at[0]
    )
    own_extra.start()

    def send_extra(target, place):
        remote(
            fan.at[target, pl.ds(0, 7)],
            extra.at[me, pl.ds(0, 7)],
            send_sem.at[0],
            recv_sem.at[0],
            place,
        ).start()

    peers.visit(send_extra)
    kept.wait()
    own_rows = None
    for dz in range(8):
        piece = pl.ds(pl.multiple_of(peers.depths[dz] * 8, 8), 8)
        across[dz].wait()
        total[:, piece, :] = (
            held[low, :, piece, :] + near[1, :, piece, :] + cross[:, piece, :]
        )
        if dz == 0:
            own_rows = pltpu.make_async_copy(
                total.at[peers.high * 8 + row, piece], got.at[me], own_sem.at[1]
            )
            own_rows.start()

        def send_rows(target, place, piece=piece):
            remote(
                total.at[target // 8, piece], got.at[me], send_sem.at[1], recv_sem.at[1], place
            ).start()

        peers.visit(send_rows, (dz,))

    def arrived(index, src, dst, size):
        everything = remote(
            src.at[pl.ds(0, GROUP - 1), pl.ds(0, size)],
            dst.at[pl.ds(0, GROUP - 1), pl.ds(0, size)],
            send_sem.at[index],
            recv_sem.at[index],
            peers.at(0, 0, 1)[1],
        )
        everything.wait_send()
        everything.wait_recv()

    own_extra.wait()
    arrived(0, fan, extra, 7)
    extra_rows = extra.reshape(GROUP * 8, NB)
    got_rows = got.reshape(GROUP * 8, NB)

    def panel_tile(slot):
        return -extra_rows[pl.ds(slot, NB, stride=8), :]

    upper, inverse = factor_and_inverse(panel_tile(6))
    lower = upper.T
    owned, crossing = [], []
    for kk in range(2):
        at_pivot = (2 * layer + kk) * 8 + row == 0
        owned.append(jnp.where(at_pivot, lower, dot_nt(panel_tile(kk), inverse)))
    for kc in range(4):
        at_pivot = kc * 16 + col == 0
        crossing.append(jnp.where(at_pivot, lower, dot_nt(panel_tile(2 + kc), inverse)))
    for kk in range(2):
        for kc in range(4):
            product = dot_nt(owned[kk], crossing[kc])
            out_ref[kk, pl.ds(kc, NB, stride=4), :] = (
                corner[kk, pl.ds(kc, NB, stride=4), :] - product
            )
    own_rows.wait()
    arrived(1, got, got, 8)
    for kk in range(2):
        for kc in range(4):
            update = got_rows[pl.ds(kk * 4 + kc, NB, stride=8), :]
            above = (2 * layer + kk) * 8 + row < kc * 16 + col
            update = jnp.where(above, update.T, update)
            result = out_ref[kk, pl.ds(kc, NB, stride=4), :] - update
            if kc == 0:
                result = jnp.where(col == 0, owned[kk], result)
            out_ref[kk, pl.ds(kc, NB, stride=4), :] = result


def shards(front_pivot, front_border, pivot_live, rows_live, border_block, row_map, separator):
    dma = pltpu.SemaphoreType.DMA
    got, side = pl.pallas_call(
        leaf_kernel,
        out_shape=[
            jax.ShapeDtypeStruct((GROUP, ROWS, NB), f32),
            jax.ShapeDtypeStruct((GROUP, 8, NB), f32),
        ],
        in_specs=[SMEM] * 3 + [VMEM] * 3 + [ANY],
        out_specs=[VMEM, VMEM],
        scratch_shapes=[
            pltpu.VMEM((GROUP, ROWS, NB), f32),
            pltpu.VMEM((GROUP, 8, NB), f32),
            pltpu.VMEM((2, NB, NB), f32),
            dma((2,)),
            dma((2,)),
            dma((2,)),
            dma,
        ],
        compiler_params=pltpu.CompilerParams(collective_id=0, has_side_effects=True),
        name="leaf",
    )(
        pivot_live,
        rows_live[0],
        border_block[0],
        row_map[0],
        front_pivot[0],
        front_border[0],
        separator,
    )
    gathered, panel = pl.pallas_call(
        collect_kernel,
        out_shape=[
            jax.ShapeDtypeStruct((4 * 1024, NB), f32),
            jax.ShapeDtypeStruct((64, NB), f32),
        ],
        in_specs=[VMEM, ANY],
        out_specs=[VMEM, VMEM],
        scratch_shapes=[pltpu.SMEM((16, 8, NB), f32), pltpu.VMEM((16, 8, NB), f32), dma((2,))],
        name="collect",
    )(got.reshape(GROUP * ROWS, NB), side.reshape(16, 8, 8, NB))
    result = pl.pallas_call(
        finish_kernel,
        out_shape=jax.ShapeDtypeStruct((2, 4 * NB, NB), f32),
        in_specs=[ANY, VMEM, ANY],
        out_specs=VMEM,
        scratch_shapes=[
            pltpu.VMEM((2, 16, 64, NB), f32),
            pltpu.VMEM((2, 4 * NB, NB), f32),
            pltpu.VMEM((2, 16, 64, NB), f32),
            pltpu.VMEM((16, 64, NB), f32),
            pltpu.VMEM((16, 64, NB), f32),
            pltpu.VMEM((16, 64, NB), f32),
            pltpu.VMEM((64, NB), f32),
            pltpu.VMEM((3, 64, NB), f32),
            pltpu.VMEM((GROUP, 8, NB), f32),
            pltpu.VMEM((GROUP, 8, NB), f32),
            pltpu.VMEM((GROUP, 8, NB), f32),
            dma((2,)),
            dma((2,)),
            dma((8,)),
            dma((8,)),
            dma((3,)),
            dma((3,)),
            dma((2,)),
            dma((2,)),
            dma((2,)),
            dma((3,)),
        ],
        compiler_params=pltpu.CompilerParams(collective_id=1, has_side_effects=True),
        name="finish",
    )(gathered.reshape(4, 16, 64, NB), panel, separator.reshape(8, 4 * NB, NB))
    return result.reshape(2, NB, 4, NB)


def solution(mesh):
    placed = (
        P(("layer", "row", "col"), None, None),
        P(("layer", "row", "col"), None, None),
        P(("layer", "row", "col")),
        P(("layer", "row", "col"), None),
        P(("layer", "row", "col"), None),
        P(("layer", "row", "col"), None, None),
        P(None, "row", None, "col"),
    )
    return jax.shard_map(
        shards,
        mesh=mesh,
        in_specs=placed,
        out_specs=P("layer", "row", None, "col"),
        check_vma=False,
    )
```

```python
import jax
import jax.numpy as jnp
from jax import lax
from jax.experimental import pallas as pl
from jax.experimental.pallas import tpu as pltpu
from jax.sharding import PartitionSpec as P

f32 = jnp.float32
highest = lax.Precision.HIGHEST
MESH = pl.DeviceIdType.MESH
NB = 128
GROUP = 128
ROWS = 16
VMEM = pl.BlockSpec(memory_space=pltpu.VMEM)
SMEM = pl.BlockSpec(memory_space=pltpu.SMEM)
ANY = pl.BlockSpec(memory_space=pl.ANY)


def dot_nt(a, b):
    return lax.dot_general(
        a, b, (((1,), (1,)), ((), ())), precision=highest, preferred_element_type=f32
    )


def dot_nn(a, b):
    return lax.dot_general(
        a, b, (((1,), (0,)), ((), ())), precision=highest, preferred_element_type=f32
    )


def factor_and_inverse(matrix):
    count = NB // 8
    lane = lax.broadcasted_iota(jnp.int32, (8, NB), 1)
    sub = lax.broadcasted_iota(jnp.int32, (8, NB), 0)

    def spread(block, s):
        return jnp.broadcast_to(block[s : s + 1, :], (8, NB))

    left = [matrix[8 * i : 8 * i + 8, :] for i in range(count)]
    right = [jnp.where(lane == sub + 8 * i, 1.0, 0.0).astype(f32) for i in range(count)]
    upper, inverse = [], []
    for t in range(count):
        columns = [
            [jnp.broadcast_to(left[i][:, 8 * t + s : 8 * t + s + 1], (8, NB)) for s in range(8)]
            for i in range(t, count)
        ]
        own = list(columns[0])
        rows, units = left[t], right[t]
        upper_rows, unit_rows, pivots = rows, units, own[0]
        for s in range(8):
            here = sub == s
            pivot = spread(own[s], s)
            scale = 1.0 / pivot
            row, unit = spread(rows, s), spread(units, s)
            upper_rows = jnp.where(here, row, upper_rows)
            unit_rows = jnp.where(here, unit, unit_rows)
            pivots = jnp.where(here, pivot, pivots)
            for j in range(s + 1, 8):
                ahead = spread(own[j], s) * scale
                own[j] = jnp.where(here, ahead, own[j] - own[s] * ahead)
            row, unit = row * scale, unit * scale
            rows = jnp.where(here, row, rows - own[s] * row)
            units = jnp.where(here, unit, units - own[s] * unit)
        for i in range(t + 1, count):
            for s in range(8):
                column = columns[i - t][s]
                left[i] = left[i] - column * spread(rows, s)
                right[i] = right[i] - column * spread(units, s)
        root = 1.0 / jnp.sqrt(pivots)
        upper.append(jnp.where(lane >= sub + 8 * t, upper_rows * root, 0.0))
        inverse.append(unit_rows * root)
    return jnp.concatenate(upper, axis=0), jnp.concatenate(inverse, axis=0)


class Peers:
    def __init__(self):
        self.layer = lax.axis_index("layer")
        self.row = lax.axis_index("row")
        self.col = lax.axis_index("col")
        self.high, self.core = self.layer // 2, lax.rem(self.layer, 2)
        self.depth, self.low = self.col // 2, lax.rem(self.col, 2)
        self.depths = [lax.rem(self.depth + dz, 8) for dz in range(8)]
        self.me = self.high * 64 + self.row * 8 + self.depth

    def at(self, dx, dy, dz):
        to_high = self.high if dx == 0 else 1 - self.high
        to_row = lax.rem(self.row + dy, 8)
        to_depth = self.depths[dz]
        place = (to_high * 2 + self.core, to_row, to_depth * 2 + self.low)
        return to_high * 64 + to_row * 8 + to_depth, place

    def visit(self, act, steps=range(8)):
        for dz in steps:
            if dz:
                act(*self.at(0, 0, dz))

        def near(dy, carry):
            for dz in steps:
                act(*self.at(0, dy, dz))
            return carry

        def far(dy, carry):
            for dz in steps:
                act(*self.at(1, dy, dz))
            return carry

        lax.fori_loop(1, 8, near, 0)
        lax.fori_loop(0, 8, far, 0)


def remote(src, dst, send_sem, recv_sem, place):
    return pltpu.make_async_remote_copy(
        src_ref=src,
        dst_ref=dst,
        send_sem=send_sem,
        recv_sem=recv_sem,
        device_id=place,
        device_id_type=MESH,
    )


def leaf_kernel(
    live_ref, rows_ref, block_ref, map_ref, pivot_ref, border_ref, sep_ref,
    got_ref, side_ref, out, early, column, send_sem, recv_sem, own_sem, column_sem,
):
    peers = Peers()
    fetch = pltpu.make_async_copy(
        sep_ref.at[pl.ds(peers.layer * 2, 2), :, 0, :], column, column_sem
    )
    fetch.start()
    barrier = pltpu.get_barrier_semaphore()

    def greet(target, place):
        pl.semaphore_signal(barrier, inc=1, device_id=place, device_id_type=MESH)

    peers.visit(greet)

    blocks = [block_ref[g] for g in range(4)]
    ranks = []
    for g in range(4):
        rank = jnp.int32(0)
        for h in range(4):
            if h != g:
                rank = rank + jnp.where(blocks[h] > blocks[g], 1, 0)
        ranks.append(rank)
    order, labels = [], []
    for s in range(4):
        g, b = jnp.int32(0), blocks[0]
        for h in range(1, 4):
            g = jnp.where(ranks[h] == s, h, g)
            b = jnp.where(ranks[h] == s, blocks[h], b)
        order.append(g)
        labels.append(b)
    lane = lax.broadcasted_iota(jnp.int32, (NB, NB), 1)
    where_row = jnp.zeros((NB, NB), jnp.int32)
    for s in range(4):
        b = labels[s]
        level = b // 16
        row_at = (level % 2) * 1024 + (level // 2) * 512 + (b % 8) * 64 + (b // 8 % 2) * 4
        col_at = (b % 2) * 2048 + (b % 16 // 2) * 8 + level
        where_row = jnp.where(lane == s, row_at, where_row)
        where_row = jnp.where(lane == 4 + s, col_at, where_row)
    early_rows = early.reshape(GROUP * 8, NB)
    early_rows[pl.ds(2, NB, stride=8), :] = where_row.astype(f32)

    live = live_ref[0]
    row = lax.broadcasted_iota(jnp.int32, (256, 256), 0)
    col = lax.broadcasted_iota(jnp.int32, (256, 256), 1)
    front = jnp.where(
        (row < live) & (col < live),
        pivot_ref[...].astype(f32),
        jnp.where(row == col, 1.0, 0.0),
    )
    first = factor_and_inverse(front[:NB, :NB])[1]

    fetch.wait()
    for k in range(2):
        early_rows[pl.ds(k, NB, stride=8), :] = column[k]
    pl.semaphore_wait(barrier, GROUP - 1)
    own_side = pltpu.make_async_copy(
        early.at[peers.me, pl.ds(0, 3)], side_ref.at[peers.me, pl.ds(0, 3)], own_sem.at[0]
    )
    own_side.start()

    def send_early(target, place):
        remote(
            early.at[target, pl.ds(0, 3)],
            side_ref.at[peers.me, pl.ds(0, 3)],
            send_sem.at[0],
            recv_sem.at[0],
            place,
        ).start()

    peers.visit(send_early)

    below = dot_nt(front[NB:, :NB], first)
    second = factor_and_inverse(front[NB:, NB:] - dot_nt(below, below))[1]
    border_row = lax.broadcasted_iota(jnp.int32, (NB, 256), 0)
    border_col = lax.broadcasted_iota(jnp.int32, (NB, 256), 1)
    home = lax.broadcasted_iota(jnp.int32, (NB, NB), 0)
    borders, placings = [], []
    for g in range(4):
        rows = border_ref[g * NB : g * NB + NB, :].astype(f32)
        keep = (border_row < rows_ref[g]) & (border_col < live)
        borders.append(jnp.where(keep, rows, 0.0))
        placings.append(jnp.where(map_ref[g : g + 1, :] == home, 1.0, 0.0).astype(f32))
    border = jnp.concatenate(borders, axis=0)
    solved_first = dot_nt(border[:, :NB], first)
    solved_second = dot_nt(border[:, NB:] - dot_nt(solved_first, below), second)
    solved = jnp.concatenate([solved_first, solved_second], axis=1)
    by_group = [dot_nn(placings[g], solved[g * NB : g * NB + NB]) for g in range(4)]
    in_order = []
    for s in range(4):
        chosen = by_group[0]
        for g in range(1, 4):
            chosen = jnp.where(order[s] == g, by_group[g], chosen)
        in_order.append(chosen)
    placed = jnp.concatenate(in_order, axis=0)
    out_rows = out.reshape(GROUP * ROWS, NB)
    slot = 0
    for s in range(4):
        tiles = dot_nt(placed[s * NB : s * NB + NB], placed[s * NB :])
        for t in range(4 - s):
            out_rows[pl.ds(slot, NB, stride=ROWS), :] = tiles[:, t * NB : t * NB + NB]
            slot += 1
    own_tiles = pltpu.make_async_copy(
        out.at[peers.me, pl.ds(0, 10)], got_ref.at[peers.me, pl.ds(0, 10)], own_sem.at[1]
    )
    own_tiles.start()

    def send_tiles(target, place):
        remote(
            out.at[target, pl.ds(0, 10)],
            got_ref.at[peers.me, pl.ds(0, 10)],
            send_sem.at[1],
            recv_sem.at[1],
            place,
        ).start()

    peers.visit(send_tiles)
    own_side.wait()
    own_tiles.wait()
    for index, src, dst, size in ((0, early, side_ref, 3), (1, out, got_ref, 10)):
        everything = remote(
            src.at[pl.ds(0, GROUP - 1), pl.ds(0, size)],
            dst.at[pl.ds(0, GROUP - 1), pl.ds(0, size)],
            send_sem.at[index],
            recv_sem.at[index],
            peers.at(0, 0, 1)[1],
        )
        everything.wait_send()
        everything.wait_recv()


def collect_kernel(got_ref, side_ref, out_ref, panel_ref, where_at, given_at, whole, column, sems):
    get_places = pltpu.make_async_copy(side_ref.at[:, :, 2, :], given_at, sems.at[0])
    get_column = pltpu.make_async_copy(side_ref.at[:, 0], column, sems.at[1])
    get_places.start()
    get_column.start()
    core_here = lax.rem(lax.axis_index("layer"), 2)
    low = lax.rem(lax.axis_index("col"), 2)

    def clear(i, carry):
        out_ref[pl.ds(pl.multiple_of(i * 128, 128), 128), :] = jnp.zeros((128, NB), f32)
        return carry

    get_places.wait()
    whole[...] = given_at[...].astype(jnp.int32)
    to_scalars = pltpu.make_async_copy(whole, where_at, sems.at[2])
    to_scalars.start()
    lax.fori_loop(0, 32, clear, 0)
    to_scalars.wait()
    get_column.wait()

    def add(leaf, carry):
        high, low_part = leaf // 8, lax.rem(leaf, 8)
        rows = [where_at[high, low_part, g] for g in range(4)]
        cols = [where_at[high, low_part, 4 + g] for g in range(4)]
        places, values = [], []
        slot = 0
        for s in range(4):
            for t in range(s, 4):
                value = got_ref[pl.ds(leaf * ROWS + slot, 1), :]
                slot += 1
                places.append(rows[s] + cols[t])
                values.append(value)
                if t > s:
                    places.append(rows[t] + cols[s])
                    values.append(value)
        before = [out_ref[pl.ds(place, 1), :] for place in places]
        for place, old, value in zip(places, before, values):
            out_ref[pl.ds(place, 1), :] = old + value
        return carry

    lax.fori_loop(0, GROUP, add, 0)
    for block in range(64):
        layer, kk, row = block // 16, (block // 8) % 2, block % 8
        high, core = layer // 2, layer % 2
        at = core * 1024 + high * 512 + row * 64 + kk * 4
        mine = jnp.where((low == 0) & (core_here == core), 1.0, 0.0)
        given = column[high * 8 + row, kk : kk + 1, :]
        panel_ref[pl.ds(block, 1), :] = out_ref[pl.ds(at, 1), :] - given * mine


def finish_kernel(
    src_ref, panel_ref, sep_ref, out_ref, held, corner, near, cross, passing, total, joined, others, fan,
    got, extra, twin_send, twin_recv, cross_send, cross_recv, panel_send, panel_recv,
    send_sem, recv_sem, own_sem, load_sem,
):
    peers = Peers()
    loads = [
        pltpu.make_async_copy(
            src_ref.at[q * 2 + peers.core], held.at[q], load_sem.at[q]
        )
        for q in range(2)
    ]
    loads.append(
        pltpu.make_async_copy(sep_ref.at[pl.ds(peers.layer * 2, 2)], corner, load_sem.at[2])
    )
    for load in loads:
        load.start()
    layer, row, col = peers.layer, peers.row, peers.col
    core, low, me = peers.core, peers.low, peers.me
    twin = (layer + 1 - 2 * core, row, col)
    beside = (layer, row, col + 1 - 2 * low)
    opposite = (layer + 1 - 2 * core, row, col + 1 - 2 * low)
    barrier = pltpu.get_barrier_semaphore()

    def greet(target, place):
        pl.semaphore_signal(barrier, inc=1, device_id=place, device_id_type=MESH)

    for place in (twin, beside, opposite):
        greet(0, place)
    peers.visit(greet)
    pl.semaphore_wait(barrier, GROUP + 2)

    panels = []
    for index, place in enumerate((twin, beside, opposite)):
        panels.append(
            remote(panel_ref, others.at[index], panel_send.at[index], panel_recv.at[index], place)
        )
    onward = remote(
        src_ref.at[(1 - low) * 2 + 1 - core], near.at[0], twin_send.at[0], twin_recv.at[0], twin
    )
    kept = remote(
        src_ref.at[low * 2 + 1 - core], near.at[1], twin_send.at[1], twin_recv.at[1], twin
    )
    for copy in (*panels, onward, kept):
        copy.start()

    for load in loads:
        load.wait()
    onward.wait()
    across = []
    for dz in range(8):
        piece = pl.ds(pl.multiple_of(peers.depths[dz] * 8, 8), 8)
        passing[:, piece, :] = held[1 - low, :, piece, :] + near[0, :, piece, :]
        across.append(
            remote(
                passing.at[:, piece],
                cross.at[:, piece],
                cross_send.at[dz],
                cross_recv.at[dz],
                beside,
            )
        )
        across[dz].start()

    for copy in panels:
        copy.wait()
    joined[...] = panel_ref[...] + others[0] + others[1] + others[2]

    def lay_out(d, carry):
        to_high, to_row, to_depth = d // 64, lax.rem(d // 8, 8), lax.rem(d, 8)
        for kk in range(2):
            block = (to_high * 2 + core) * 16 + kk * 8 + to_row
            fan[d, kk : kk + 1, :] = joined[pl.ds(block, 1), :]
        for kc in range(4):
            block = kc * 16 + to_depth * 2 + low
            fan[d, 2 + kc : 3 + kc, :] = joined[pl.ds(block, 1), :]
        fan[d, 6:7, :] = joined[0:1, :]
        return carry

    lax.fori_loop(0, GROUP, lay_out, 0)
    own_extra = pltpu.make_async_copy(
        fan.at[me, pl.ds(0, 7)], extra.at[me, pl.ds(0, 7)], own_sem.at[0]
    )
    own_extra.start()

    def send_extra(target, place):
        remote(
            fan.at[target, pl.ds(0, 7)],
            extra.at[me, pl.ds(0, 7)],
            send_sem.at[0],
            recv_sem.at[0],
            place,
        ).start()

    peers.visit(send_extra)
    kept.wait()
    own_rows = None
    for dz in range(8):
        piece = pl.ds(pl.multiple_of(peers.depths[dz] * 8, 8), 8)
        across[dz].wait()
        total[:, piece, :] = (
            held[low, :, piece, :] + near[1, :, piece, :] + cross[:, piece, :]
        )
        if dz == 0:
            own_rows = pltpu.make_async_copy(
                total.at[peers.high * 8 + row, piece], got.at[me], own_sem.at[1]
            )
            own_rows.start()

        def send_rows(target, place, piece=piece):
            remote(
                total.at[target // 8, piece], got.at[me], send_sem.at[1], recv_sem.at[1], place
            ).start()

        peers.visit(send_rows, (dz,))

    def arrived(index, src, dst, size):
        everything = remote(
            src.at[pl.ds(0, GROUP - 1), pl.ds(0, size)],
            dst.at[pl.ds(0, GROUP - 1), pl.ds(0, size)],
            send_sem.at[index],
            recv_sem.at[index],
            peers.at(0, 0, 1)[1],
        )
        everything.wait_send()
        everything.wait_recv()

    own_extra.wait()
    arrived(0, fan, extra, 7)
    extra_rows = extra.reshape(GROUP * 8, NB)
    got_rows = got.reshape(GROUP * 8, NB)

    def panel_tile(slot):
        return -extra_rows[pl.ds(slot, NB, stride=8), :]

    upper, inverse = factor_and_inverse(panel_tile(6))
    lower = upper.T
    owned, crossing = [], []
    for kk in range(2):
        at_pivot = (2 * layer + kk) * 8 + row == 0
        owned.append(jnp.where(at_pivot, lower, dot_nt(panel_tile(kk), inverse)))
    for kc in range(4):
        at_pivot = kc * 16 + col == 0
        crossing.append(jnp.where(at_pivot, lower, dot_nt(panel_tile(2 + kc), inverse)))
    for kk in range(2):
        for kc in range(4):
            product = dot_nt(owned[kk], crossing[kc])
            out_ref[kk, pl.ds(kc, NB, stride=4), :] = (
                corner[kk, pl.ds(kc, NB, stride=4), :] - product
            )
    own_rows.wait()
    arrived(1, got, got, 8)
    for kk in range(2):
        for kc in range(4):
            update = got_rows[pl.ds(kk * 4 + kc, NB, stride=8), :]
            above = (2 * layer + kk) * 8 + row < kc * 16 + col
            update = jnp.where(above, update.T, update)
            result = out_ref[kk, pl.ds(kc, NB, stride=4), :] - update
            if kc == 0:
                result = jnp.where(col == 0, owned[kk], result)
            out_ref[kk, pl.ds(kc, NB, stride=4), :] = result


def shards(front_pivot, front_border, pivot_live, rows_live, border_block, row_map, separator):
    dma = pltpu.SemaphoreType.DMA
    got, side = pl.pallas_call(
        leaf_kernel,
        out_shape=[
            jax.ShapeDtypeStruct((GROUP, ROWS, NB), f32),
            jax.ShapeDtypeStruct((GROUP, 8, NB), f32),
        ],
        in_specs=[SMEM] * 3 + [VMEM] * 3 + [ANY],
        out_specs=[VMEM, VMEM],
        scratch_shapes=[
            pltpu.VMEM((GROUP, ROWS, NB), f32),
            pltpu.VMEM((GROUP, 8, NB), f32),
            pltpu.VMEM((2, NB, NB), f32),
            dma((2,)),
            dma((2,)),
            dma((2,)),
            dma,
        ],
        compiler_params=pltpu.CompilerParams(collective_id=0, has_side_effects=True),
        name="leaf",
    )(
        pivot_live,
        rows_live[0],
        border_block[0],
        row_map[0],
        front_pivot[0],
        front_border[0],
        separator,
    )
    gathered, panel = pl.pallas_call(
        collect_kernel,
        out_shape=[
            jax.ShapeDtypeStruct((4 * 1024, NB), f32),
            jax.ShapeDtypeStruct((64, NB), f32),
        ],
        in_specs=[VMEM, ANY],
        out_specs=[VMEM, VMEM],
        scratch_shapes=[
            pltpu.SMEM((16, 8, NB), jnp.int32),
            pltpu.VMEM((16, 8, NB), f32),
            pltpu.VMEM((16, 8, NB), jnp.int32),
            pltpu.VMEM((16, 8, NB), f32),
            dma((3,)),
        ],
        name="collect",
    )(got.reshape(GROUP * ROWS, NB), side.reshape(16, 8, 8, NB))
    result = pl.pallas_call(
        finish_kernel,
        out_shape=jax.ShapeDtypeStruct((2, 4 * NB, NB), f32),
        in_specs=[ANY, VMEM, ANY],
        out_specs=VMEM,
        scratch_shapes=[
            pltpu.VMEM((2, 16, 64, NB), f32),
            pltpu.VMEM((2, 4 * NB, NB), f32),
            pltpu.VMEM((2, 16, 64, NB), f32),
            pltpu.VMEM((16, 64, NB), f32),
            pltpu.VMEM((16, 64, NB), f32),
            pltpu.VMEM((16, 64, NB), f32),
            pltpu.VMEM((64, NB), f32),
            pltpu.VMEM((3, 64, NB), f32),
            pltpu.VMEM((GROUP, 8, NB), f32),
            pltpu.VMEM((GROUP, 8, NB), f32),
            pltpu.VMEM((GROUP, 8, NB), f32),
            dma((2,)),
            dma((2,)),
            dma((8,)),
            dma((8,)),
            dma((3,)),
            dma((3,)),
            dma((2,)),
            dma((2,)),
            dma((2,)),
            dma((3,)),
        ],
        compiler_params=pltpu.CompilerParams(collective_id=1, has_side_effects=True),
        name="finish",
    )(gathered.reshape(4, 16, 64, NB), panel, separator.reshape(8, 4 * NB, NB))
    return result.reshape(2, NB, 4, NB)


def solution(mesh):
    placed = (
        P(("layer", "row", "col"), None, None),
        P(("layer", "row", "col"), None, None),
        P(("layer", "row", "col")),
        P(("layer", "row", "col"), None),
        P(("layer", "row", "col"), None),
        P(("layer", "row", "col"), None, None),
        P(None, "row", None, "col"),
    )
    return jax.shard_map(
        shards,
        mesh=mesh,
        in_specs=placed,
        out_specs=P("layer", "row", None, "col"),
        check_vma=False,
    )
```
